32 devices in a mesh: kpt: 2 (over x), grid: 16 (over z, y, core).
Axes of the slice: x: 2, y: 2, z: 4, core: 2. Of those that a mesh axis runs over, the one named last changes fastest.
Arguments:
- orbitals: bfloat16 [4, 2, 2, 512, 256, 256], P('kpt', None, None, 'grid'), may hold values from -6 to 6
- kweights: int32 [4], P('kpt'), may hold values from 1 to 16
- occupations: int32 [4, 2], P('kpt'), may hold values from 0 to 2
- z_basis: float32 [512, 512], replicated, may hold values from -0.25 to 0.25
- z_eigen: float32 [512], replicated, may hold values from 0.25 to 4
Outputs:
- potential: float32 [512, 256, 256], P('grid')
The draws below stay inside these ranges and needn't reach their ends.
All inputs are finite; a program needn't handle non-finite values.
Results may differ from the reference program's by a relative error of at most 0.0003.
Values sent between devices are 32-bit elements; how exact they have to be, the bound alone decides.
No kernel may reach another device: no remote copies, remote signals or barrier semaphores. Data moves between devices by JAX's collectives and lax.ppermute only.
A program may use at most 128 MiB of HBM per device.

```python
import math
import jax
import jax.numpy as jnp
from jax import lax

NX = 256
NY = 256
NZ = 512
KPD = 2
BANDS = 2
KPOINTS = 4


def draw_kweights(key, part):
    first, second = jax.random.split(jax.random.fold_in(key, 11))
    base = jax.random.randint(first, (KPOINTS,), 1, 17)
    chosen = jax.random.randint(second, (), 0, KPOINTS)
    places = jnp.arange(KPOINTS, dtype=jnp.int32)
    return jnp.where(places == chosen, 16, base).astype(jnp.int32)


def draw_occupations(key, part):
    first, second = jax.random.split(jax.random.fold_in(key, 23))
    base = jax.random.randint(first, (KPOINTS * BANDS,), 0, 3)
    order = jax.random.permutation(second, KPOINTS * BANDS)
    mixed = jnp.where(order == 0, 0, jnp.where(order == 1, 2, base))
    return mixed.reshape(KPOINTS, BANDS).astype(jnp.int32)


def block_scale(own_key, extent, shards, low, top_value):
    def one(position, blocks):
        steps = jax.random.uniform(jax.random.fold_in(jax.random.fold_in(own_key, 6), position), (blocks,), jnp.float32, low / len(shards), top_value / len(shards))
        return jnp.repeat(jnp.exp(steps), extent[position] // blocks).reshape((-1,) + (1,) * (len(extent) - position - 1))

    loudness = one(*shards[0])
    for cut in shards[1:]:
        loudness = loudness * one(*cut)
    return loudness


def scatter_about(own_key, extent, scale, most, cuts=(), held_as=jnp.bfloat16):
    level = block_scale(own_key, extent, cuts, -0.22, 0.18) if cuts else 1.0
    values = jax.random.normal(own_key, extent, jnp.float32) * scale * level
    return jnp.minimum(jnp.maximum(values, -most), most).astype(held_as)


def setup_inputs(seed: int = 0) -> dict:
    keys = jax.random.split(jax.random.key(seed), 6)
    orbitals = scatter_about(keys[0], (KPOINTS, BANDS, 2, NZ, NX, NY), 1.0, 6.0, ((0, 2), (3, 16)))
    kweights = draw_kweights(jax.random.fold_in(keys[5], 71), 0)
    occupations = draw_occupations(jax.random.fold_in(keys[5], 71), 0)
    z_basis = scatter_about(keys[3], (NZ, NZ), NZ ** -0.5, 0.25, (), jnp.float32)
    z_eigen = jnp.clip(jnp.exp(jax.random.uniform(keys[4], (NZ,), jnp.float32, math.log(0.25), math.log(4.0))), 0.25, 4.0)
    return {"orbitals": orbitals, "kweights": kweights, "occupations": occupations, "z_basis": z_basis, "z_eigen": z_eigen}


precise = lax.Precision.HIGHEST


def reference(orbitals, kweights, occupations, z_basis, z_eigen):
    factor = (kweights[:, None] * occupations).astype(jnp.float32) / (16.0 * KPD * BANDS)

    def add_point(kpoint, running):
        values = lax.dynamic_index_in_dim(orbitals, kpoint, 0, keepdims=False).astype(jnp.float32)
        weights = lax.dynamic_index_in_dim(factor, kpoint, 0, keepdims=False)
        return running + jnp.sum(weights[:, None, None, None, None] * values * values, axis=(0, 1))

    density = lax.fori_loop(0, KPOINTS, add_point, jnp.zeros((NZ, NX, NY), jnp.float32))
    spectrum = jnp.fft.fft2(density, axes=(1, 2))
    stacked = jnp.stack([jnp.real(spectrum), jnp.imag(spectrum)]).astype(jnp.float32)
    wave_x = jnp.arange(NX).astype(jnp.float32)
    wave_y = jnp.arange(NY).astype(jnp.float32)
    shift_x = 2.0 * jnp.sin(jnp.pi * wave_x / NX)
    shift_y = 2.0 * jnp.sin(jnp.pi * wave_y / NY)
    shifted = shift_x[:, None] ** 2 + shift_y[None, :] ** 2
    factors = 1.0 / (z_eigen[:, None, None] + shifted[None])
    projected = jnp.einsum('zj,czab->cjab', z_basis, stacked, precision=precise)
    filtered = jnp.einsum('zj,cjab->czab', z_basis, projected * factors[None], precision=precise)
    potential = jnp.fft.ifft2(lax.complex(filtered[0], filtered[1]), axes=(1, 2))
    return jnp.real(potential).astype(jnp.float32)
```

```python
import numpy as np
import jax
import jax.numpy as jnp
from jax import lax
from jax.experimental import pallas as pl
from jax.experimental.pallas import tpu as pltpu
from jax.sharding import PartitionSpec as P


f32 = jnp.float32
bf16 = jnp.bfloat16


def real_basis(length):
    position = np.arange(length)
    angles = (position[:, None] * position[None, :] % length) * (2.0 * np.pi / length)
    table = np.where(position[:, None] <= length // 2, np.cos(angles), np.sin(angles))
    edges = (position == 0) | (position == length // 2)
    weights = np.where(edges, 1.0, 2.0) / length
    return table.astype(np.float32), (table * weights[:, None]).astype(np.float32)


def split_const(table):
    high = table.astype(jnp.bfloat16)
    low = (table - high.astype(np.float32)).astype(jnp.bfloat16)
    return jnp.asarray(high), jnp.asarray(low)


def split(value):
    high = value.astype(bf16)
    return high, (value - high.astype(f32)).astype(bf16)


def dot3(ah, al, bh, bl):
    def one(a, b):
        return jnp.dot(a, b, preferred_element_type=f32)

    return one(ah, bh) + (one(ah, bl) + one(al, bh))


def whole(shape):
    zeros = (0,) * len(shape)
    return pl.BlockSpec(shape, lambda *_: zeros)


def smem():
    return pl.BlockSpec(memory_space=pltpu.SMEM)


def cost(flops, bytes_accessed):
    return pl.CostEstimate(flops=int(flops), bytes_accessed=int(bytes_accessed), transcendentals=0)


GROUP = 8


def forward(orbitals, kweights, occupations, half, tables, chunk, blocks, step=2):
    points, bands, parts, _, nx, ny = orbitals.shape
    rows = nx // (2 * blocks)
    steps = GROUP // step
    scale = 1.0 / (16.0 * points * bands)

    def body(half_ref, kweights_ref, occ_ref, orb_ref, yh_ref, yl_ref, xh_ref, xl_ref, own_ref, other_ref, s_ref):
        mine = half_ref[0]
        here = pl.program_id(0)
        yh, yl = yh_ref[...], yl_ref[...]
        for plane in range(step):
            total = None
            for point in range(points):
                for band in range(bands):
                    weight = (kweights_ref[point] * occ_ref[point, band]).astype(f32) * scale
                    real = orb_ref[point, band, 0, plane].astype(f32)
                    imag = orb_ref[point, band, 1, plane].astype(f32)
                    term = weight * (real * real + imag * imag)
                    total = term if total is None else total + term
            dh, dl = split(total)
            ah, al = split(dot3(dh, dl, yh, yl))
            s_ref[here * step + plane] = dot3(xh_ref[...], xl_ref[...], ah, al)

        @pl.when(here == steps - 1)
        def _():
            for slot, out in ((0, own_ref), (1, other_ref)):
                first = pl.multiple_of((mine if slot == 0 else 1 - mine) * (nx // 2), nx // 2)
                for plane in range(GROUP):
                    out[:, :, plane, :] = s_ref[plane, pl.ds(first, nx // 2), :].reshape(blocks, rows, ny)

    out_shape = jax.ShapeDtypeStruct((blocks, rows, GROUP, ny), f32)
    return pl.pallas_call(
        body,
        grid=(steps,),
        in_specs=[smem(), smem(), smem()]
        + [pl.BlockSpec((points, bands, parts, step, nx, ny), lambda i: (0, 0, 0, chunk * steps + i, 0, 0))]
        + [whole(t.shape) for t in tables],
        out_specs=[whole(out_shape.shape)] * 2,
        out_shape=[out_shape] * 2,
        scratch_shapes=[pltpu.VMEM((GROUP, nx, ny), f32)],
        cost_estimate=cost(GROUP * 12 * nx * ny * nx, GROUP * nx * ny * 24),
        name="forward",
    )(half, kweights, occupations, orbitals, *tables)


def prepare(z_basis, blocks, planes):
    nz = z_basis.shape[0]
    chunks = planes // GROUP
    size = blocks * GROUP

    def body(z_ref, zh_ref, zl_ref, th_ref, tl_ref):
        value = z_ref[...].reshape(size, nz)
        zh_ref[0], zl_ref[0] = split(value)
        th_ref[0], tl_ref[0] = split(value.T)

    straight = jax.ShapeDtypeStruct((chunks, size, nz), bf16)
    turned = jax.ShapeDtypeStruct((chunks, nz, size), bf16)
    return pl.pallas_call(
        body,
        grid=(chunks,),
        in_specs=[pl.BlockSpec((blocks, GROUP, nz), lambda i: (0, i, 0))],
        out_specs=[pl.BlockSpec((1, size, nz), lambda i: (i, 0, 0))] * 2 + [pl.BlockSpec((1, nz, size), lambda i: (i, 0, 0))] * 2,
        out_shape=[straight] * 2 + [turned] * 2,
        cost_estimate=cost(nz * nz * 100, nz * nz * 12),
        name="prepare",
    )(z_basis.reshape(blocks, planes, nz))


def by_row(blocks, ny):
    return pl.BlockSpec((blocks, 1, GROUP, ny), lambda i: (0, i, 0, 0))


def one_chunk(table, chunk):
    return pl.BlockSpec((1,) + table.shape[1:], lambda i: (chunk, 0, 0))


def project(columns, turned, chunk, before):
    blocks, rows, _, ny = columns.shape
    nz = turned[0].shape[1]
    size = blocks * GROUP
    extra = () if before is None else (before,)

    def body(x_ref, th_ref, tl_ref, *refs):
        xh, xl = split(x_ref[:, 0].reshape(size, ny))
        value = dot3(th_ref[0], tl_ref[0], xh, xl)
        refs[-1][0] = value if before is None else value + refs[0][0]

    part = pl.BlockSpec((1, nz, ny), lambda i: (i, 0, 0))
    return pl.pallas_call(
        body,
        grid=(rows,),
        in_specs=[by_row(blocks, ny)] + [one_chunk(t, chunk) for t in turned] + [part for _ in extra],
        out_specs=part,
        out_shape=jax.ShapeDtypeStruct((rows, nz, ny), f32),
        cost_estimate=cost(6 * nz * size * rows * ny, 8 * nz * rows * ny),
        name="project",
    )(columns, *turned, *extra)


def solve(part, columns, straight, turned, eigen, shift, chunk):
    blocks, rows, _, ny = columns.shape
    nz = turned[0].shape[1]
    size = blocks * GROUP

    def body(part_ref, x_ref, th_ref, tl_ref, zh_ref, zl_ref, e_ref, s_ref, out_ref, wh_ref, wl_ref):
        xh, xl = split(x_ref[:, 0].reshape(size, ny))
        projected = part_ref[0] + dot3(th_ref[0], tl_ref[0], xh, xl)
        wh, wl = split(projected / (e_ref[...] + s_ref[0]))
        wh_ref[0], wl_ref[0] = wh, wl
        out_ref[:, 0] = dot3(zh_ref[0], zl_ref[0], wh, wl).reshape(blocks, GROUP, ny)

    w_spec = pl.BlockSpec((1, nz, ny), lambda i: (i, 0, 0))
    w_shape = jax.ShapeDtypeStruct((rows, nz, ny), bf16)
    return pl.pallas_call(
        body,
        grid=(rows,),
        in_specs=[w_spec, by_row(blocks, ny)]
        + [one_chunk(t, chunk) for t in turned]
        + [one_chunk(z, 0) for z in straight]
        + [whole(eigen.shape), pl.BlockSpec((1, 1, ny), lambda i: (i, 0, 0))],
        out_specs=[by_row(blocks, ny), w_spec, w_spec],
        out_shape=[jax.ShapeDtypeStruct(columns.shape, f32), w_shape, w_shape],
        cost_estimate=cost(12 * nz * rows * ny * size, 12 * nz * rows * ny),
        name="solve",
    )(part, columns, *turned, *straight, eigen, shift)


def filtered(wh, wl, straight, chunk, blocks):
    rows, nz, ny = wh.shape

    def body(wh_ref, wl_ref, zh_ref, zl_ref, out_ref):
        out_ref[:, 0] = dot3(zh_ref[0], zl_ref[0], wh_ref[0], wl_ref[0]).reshape(blocks, GROUP, ny)

    w_spec = pl.BlockSpec((1, nz, ny), lambda i: (i, 0, 0))
    return pl.pallas_call(
        body,
        grid=(rows,),
        in_specs=[w_spec, w_spec] + [one_chunk(z, chunk) for z in straight],
        out_specs=by_row(blocks, ny),
        out_shape=jax.ShapeDtypeStruct((blocks, rows, GROUP, ny), f32),
        cost_estimate=cost(6 * nz * rows * ny * blocks * GROUP, 4 * nz * rows * ny),
        name="filtered",
    )(wh, wl, *straight)


def inverse(own, other, half, tables, planes, chunk, into, step=2):
    blocks, rows, _, ny = own.shape
    nx = 2 * blocks * rows
    steps = GROUP // step
    extra = () if into is None else (into,)

    def body(half_ref, own_ref, other_ref, yh_ref, yl_ref, xh_ref, xl_ref, *refs):
        out_ref, f_ref = refs[-2:]
        here = pl.program_id(0)

        @pl.when(here == 0)
        def _():
            for slot, ref in ((0, own_ref), (1, other_ref)):
                first = pl.multiple_of((half_ref[0] if slot == 0 else 1 - half_ref[0]) * (nx // 2), nx // 2)
                for plane in range(GROUP):
                    f_ref[plane, pl.ds(first, nx // 2), :] = ref[:, :, plane, :].reshape(nx // 2, ny)

        for plane in range(step):
            fh, fl = split(f_ref[here * step + plane])
            hh, hl = split(dot3(fh, fl, yh_ref[...], yl_ref[...]))
            out_ref[plane] = dot3(xh_ref[...], xl_ref[...], hh, hl)

    operands = (half, own, other, *tables, *extra)
    return pl.pallas_call(
        body,
        grid=(steps,),
        in_specs=[smem(), whole(own.shape), whole(other.shape)]
        + [whole(t.shape) for t in tables]
        + [pl.BlockSpec(memory_space=pl.ANY) for _ in extra],
        out_specs=pl.BlockSpec((step, nx, ny), lambda i: (chunk * steps + i, 0, 0)),
        out_shape=jax.ShapeDtypeStruct((planes, nx, ny), f32),
        scratch_shapes=[pltpu.VMEM((GROUP, nx, ny), f32)],
        input_output_aliases={len(operands) - 1: 0} if extra else {},
        cost_estimate=cost(GROUP * 12 * nx * ny * nx, GROUP * nx * ny * 8),
        name="inverse",
    )(*operands)


def row_shift(first, rows, nx, ny):
    wave_x = (first + jnp.arange(rows, dtype=jnp.int32)).astype(f32)
    wave_y = jnp.arange(ny, dtype=jnp.int32).astype(f32)
    shift_x = 2.0 * jnp.sin(jnp.pi * wave_x / nx)
    shift_y = 2.0 * jnp.sin(jnp.pi * wave_y / ny)
    return shift_x[:, None] ** 2 + shift_y[None, :] ** 2


def swap(value):
    return lax.ppermute(value, "kpt", [(0, 1), (1, 0)])


def exchange(value):
    return lax.all_to_all(value, "grid", split_axis=0, concat_axis=0, tiled=True)


def on_device_kernels(orbitals, kweights, occupations, z_basis, z_eigen):
    planes, nx, ny = orbitals.shape[3:]
    blocks = lax.axis_size("grid")
    rows = nx // (2 * blocks)
    chunks = planes // GROUP
    mine = lax.axis_index("kpt").astype(jnp.int32)
    half = mine.reshape(1)
    table_x, scaled_x = real_basis(nx)
    table_y, scaled_y = real_basis(ny)
    to_modes = (*split_const(np.ascontiguousarray(table_y.T)), *split_const(table_x))
    to_grid = (*split_const(scaled_y), *split_const(np.ascontiguousarray(scaled_x.T)))

    columns = []
    for chunk in range(chunks):
        own, other = forward(orbitals, kweights, occupations, half, to_modes, chunk, blocks)
        if chunk == 0:
            z_basis, z_eigen, own = lax.optimization_barrier((z_basis, z_eigen, own))
        other = swap(other)
        own = own + other
        columns.append(exchange(own))
    zh, zl, th, tl = prepare(z_basis, blocks, planes)
    first = (mine * blocks + lax.axis_index("grid")) * rows
    shift = row_shift(first, rows, nx, ny)[:, None, :]
    part = None
    for chunk in range(chunks - 1):
        part = project(columns[chunk], (th, tl), chunk, part)
    if part is None:
        part = jnp.zeros((rows, planes * blocks, ny), f32)
    ready, wh, wl = solve(part, columns[-1], (zh, zl), (th, tl), z_eigen[:, None], shift, chunks - 1)
    out = None
    for chunk in range(chunks):
        ready = ready if chunk == 0 else filtered(wh, wl, (zh, zl), chunk, blocks)
        own = exchange(ready)
        other = swap(own)
        out = inverse(own, other, half, to_grid, planes, chunk, out)
    return out


precise = lax.Precision.HIGHEST


def on_device_plain(orbitals, kweights, occupations, z_basis, z_eigen):
    points, bands, _, planes, nx, ny = orbitals.shape
    blocks = lax.axis_size("grid")
    rows = nx // (2 * blocks)
    nz = planes * blocks
    mine = lax.axis_index("kpt")
    weights = (kweights[:, None] * occupations).astype(f32) / (16.0 * points * bands)
    values = orbitals.astype(f32)
    density = jnp.sum(weights[:, :, None, None, None, None] * values * values, axis=(0, 1, 2))
    table_x, scaled_x = (jnp.roll(jnp.asarray(t), -mine * (nx // 2), axis=0) for t in real_basis(nx))
    table_y, scaled_y = real_basis(ny)
    along = jnp.einsum("zxy,ky->zxk", density, table_y, precision=precise)
    spectrum = jnp.einsum("jx,zxk->jzk", table_x, along, precision=precise).reshape(2, blocks, rows, planes, ny)
    columns = exchange(spectrum[0] + swap(spectrum[1]))
    first = (mine * blocks + lax.axis_index("grid")) * rows
    factors = 1.0 / (z_eigen[:, None, None] + row_shift(first, rows, nx, ny)[None])
    by_plane = z_basis.reshape(blocks, planes, nz)
    projected = jnp.einsum("gpj,gapk->jak", by_plane, columns, precision=precise)
    filtered = jnp.einsum("gpj,jak->gapk", by_plane, projected * factors, precision=precise)
    own = exchange(filtered)
    modes = jnp.stack([own, swap(own)]).reshape(nx, planes, ny)
    half_done = jnp.einsum("jx,jzk->zxk", scaled_x, modes, precision=precise)
    return jnp.einsum("zxk,ky->zxy", half_done, scaled_y, precision=precise)


def whole_tiles(shape, blocks):
    planes, nx, ny = shape[3:]
    rows = nx // (2 * blocks)
    return rows % 8 == 0 and ny % 128 == 0 and nx % 256 == 0 and planes % GROUP == 0


def on_device(orbitals, *rest):
    if not whole_tiles(orbitals.shape, lax.axis_size("grid")):
        return on_device_plain(orbitals, *rest)
    return on_device_kernels(orbitals, *rest)


def solution(mesh):
    step = jax.shard_map(
        on_device,
        mesh=mesh,
        in_specs=(P("kpt", None, None, "grid", None, None), P("kpt"), P("kpt", None), P(), P()),
        out_specs=P("grid", None, None),
        check_vma=False,
    )

    def run(orbitals, *rest):
        blocks = mesh.shape["grid"]
        local = list(orbitals.shape)
        local[3] //= blocks
        if not whole_tiles(local, blocks):
            return step(orbitals, *rest)
        return step(orbitals, *rest)

    return run
```

```python
import numpy as np
import jax
import jax.numpy as jnp
from jax import lax
from jax.experimental import pallas as pl
from jax.experimental.pallas import tpu as pltpu
from jax.sharding import PartitionSpec as P


f32 = jnp.float32
bf16 = jnp.bfloat16


def real_basis(length):
    position = np.arange(length)
    angles = (position[:, None] * position[None, :] % length) * (2.0 * np.pi / length)
    table = np.where(position[:, None] <= length // 2, np.cos(angles), np.sin(angles))
    edges = (position == 0) | (position == length // 2)
    weights = np.where(edges, 1.0, 2.0) / length
    return table.astype(np.float32), (table * weights[:, None]).astype(np.float32)


def split_const(table):
    high = table.astype(jnp.bfloat16)
    low = (table - high.astype(np.float32)).astype(jnp.bfloat16)
    return jnp.asarray(high), jnp.asarray(low)


def split(value):
    high = value.astype(bf16)
    return high, (value - high.astype(f32)).astype(bf16)


def dot3(ah, al, bh, bl):
    def one(a, b):
        return jnp.dot(a, b, preferred_element_type=f32)

    return one(ah, bh) + (one(ah, bl) + one(al, bh))


def whole(shape):
    zeros = (0,) * len(shape)
    return pl.BlockSpec(shape, lambda *_: zeros)


def smem():
    return pl.BlockSpec(memory_space=pltpu.SMEM)


def cost(flops, bytes_accessed):
    return pl.CostEstimate(flops=int(flops), bytes_accessed=int(bytes_accessed), transcendentals=0)


GROUP = 8
INNER = 4


def forward(orbitals, kweights, occupations, half, tables, chunk, blocks, plain, step=2):
    points, bands, parts, _, nx, ny = orbitals.shape
    rows = nx // (2 * blocks)
    steps = GROUP // step
    scale = 1.0 / (16.0 * points * bands)

    def body(half_ref, kweights_ref, occ_ref, orb_ref, yh_ref, yl_ref, xh_ref, xl_ref, own_ref, other_ref, s_ref):
        mine, place = half_ref[0], half_ref[1]
        here = pl.program_id(0)
        yh, yl = yh_ref[...], yl_ref[...]
        for plane in range(step):
            total = None
            for point in range(points):
                for band in range(bands):
                    weight = (kweights_ref[point] * occ_ref[point, band]).astype(f32) * scale
                    real = orb_ref[point, band, 0, plane].astype(f32)
                    imag = orb_ref[point, band, 1, plane].astype(f32)
                    term = weight * (real * real + imag * imag)
                    total = term if total is None else total + term
            dh, dl = split(total)
            ah, al = split(dot3(dh, dl, yh, yl))
            s_ref[here * step + plane] = dot3(xh_ref[...], xl_ref[...], ah, al)

        @pl.when(here == steps - 1)
        def _():
            for slot, out in ((0, own_ref), (1, other_ref)):
                for block in range(blocks):
                    first = ((mine if slot == 0 else 1 - mine) * blocks + (block if plain else place ^ block)) * rows
                    for plane in range(GROUP):
                        out[block, :, plane, :] = s_ref[plane, pl.ds(pl.multiple_of(first, rows), rows), :]

    out_shape = jax.ShapeDtypeStruct((blocks, rows, GROUP, ny), f32)
    return pl.pallas_call(
        body,
        grid=(steps,),
        in_specs=[smem(), smem(), smem()]
        + [pl.BlockSpec((points, bands, parts, step, nx, ny), lambda i: (0, 0, 0, chunk * steps + i, 0, 0))]
        + [whole(t.shape) for t in tables],
        out_specs=[whole(out_shape.shape)] * 2,
        out_shape=[out_shape] * 2,
        scratch_shapes=[pltpu.VMEM((GROUP, nx, ny), f32)],
        cost_estimate=cost(GROUP * 12 * nx * ny * nx, GROUP * nx * ny * 24),
        name="forward",
    )(half, kweights, occupations, orbitals, *tables)


def prepare(z_basis, half, blocks, planes):
    nz = z_basis.shape[0]
    chunks = planes // GROUP
    size = blocks * GROUP

    def body(half_ref, z_ref, zh_ref, zl_ref, th_ref, tl_ref):
        order = [outer * INNER + inner for inner in range(INNER) for outer in range(blocks // INNER)]
        here = pl.program_id(0)

        def rows_of(plain):
            places = [jnp.where(plain, n, half_ref[1] ^ block) for n, block in enumerate(order)]
            return jnp.concatenate([z_ref[place] for place in places], axis=0)

        zh_ref[0], zl_ref[0] = split(rows_of(here == 0))
        th_ref[0], tl_ref[0] = split(rows_of(here == chunks - 1).T)

    straight = jax.ShapeDtypeStruct((chunks, size, nz), bf16)
    turned = jax.ShapeDtypeStruct((chunks, nz, size), bf16)
    return pl.pallas_call(
        body,
        grid=(chunks,),
        in_specs=[smem(), pl.BlockSpec((blocks, GROUP, nz), lambda i: (0, i, 0))],
        out_specs=[pl.BlockSpec((1, size, nz), lambda i: (i, 0, 0))] * 2 + [pl.BlockSpec((1, nz, size), lambda i: (i, 0, 0))] * 2,
        out_shape=[straight] * 2 + [turned] * 2,
        cost_estimate=cost(nz * nz * 100, nz * nz * 12),
        name="prepare",
    )(half, z_basis.reshape(blocks, planes, nz))


def by_row(part):
    return pl.BlockSpec((part.shape[0], 1) + part.shape[2:], lambda i: (0, i, 0, 0))


def gather_row(refs, ny):
    return jnp.concatenate([ref[:, 0].reshape(-1, ny) for ref in refs], axis=0)


def scatter_row(refs, value):
    first = 0
    for ref in refs:
        size = ref.shape[0] * GROUP
        ref[:, 0] = value[first : first + size].reshape(ref.shape[0], GROUP, value.shape[1])
        first += size


def one_chunk(table, chunk):
    return pl.BlockSpec((1,) + table.shape[1:], lambda i: (chunk, 0, 0))


def project(columns, turned, chunk, before):
    rows, _, ny = columns[0].shape[1:]
    nz, size = turned[0].shape[1:]
    many = len(columns)
    extra = () if before is None else (before,)

    def body(*refs):
        xh, xl = split(gather_row(refs[:many], ny))
        value = dot3(refs[many][0], refs[many + 1][0], xh, xl)
        refs[-1][0] = value if before is None else value + refs[many + 2][0]

    part = pl.BlockSpec((1, nz, ny), lambda i: (i, 0, 0))
    return pl.pallas_call(
        body,
        grid=(rows,),
        in_specs=[by_row(c) for c in columns] + [one_chunk(t, chunk) for t in turned] + [part for _ in extra],
        out_specs=part,
        out_shape=jax.ShapeDtypeStruct((rows, nz, ny), f32),
        cost_estimate=cost(6 * nz * size * rows * ny, 8 * nz * rows * ny),
        name="project",
    )(*columns, *turned, *extra)


def solve(part, columns, straight, turned, eigen, shift, chunk):
    rows, _, ny = columns[0].shape[1:]
    nz, size = turned[0].shape[1:]
    many = len(columns)

    def body(part_ref, *refs):
        th_ref, tl_ref, zh_ref, zl_ref, e_ref, s_ref = refs[many : many + 6]
        wh_ref, wl_ref = refs[-2:]
        xh, xl = split(gather_row(refs[:many], ny))
        projected = part_ref[0] + dot3(th_ref[0], tl_ref[0], xh, xl)
        wh, wl = split(projected / (e_ref[...] + s_ref[0]))
        wh_ref[0], wl_ref[0] = wh, wl
        scatter_row(refs[many + 6 : -2], dot3(zh_ref[0], zl_ref[0], wh, wl))

    w_spec = pl.BlockSpec((1, nz, ny), lambda i: (i, 0, 0))
    w_shape = jax.ShapeDtypeStruct((rows, nz, ny), bf16)
    *ready, wh, wl = pl.pallas_call(
        body,
        grid=(rows,),
        in_specs=[w_spec]
        + [by_row(c) for c in columns]
        + [one_chunk(t, chunk) for t in turned]
        + [one_chunk(z, 0) for z in straight]
        + [whole(eigen.shape), pl.BlockSpec((1, 1, ny), lambda i: (i, 0, 0))],
        out_specs=[by_row(c) for c in columns] + [w_spec, w_spec],
        out_shape=[jax.ShapeDtypeStruct(c.shape, f32) for c in columns] + [w_shape, w_shape],
        cost_estimate=cost(12 * nz * rows * ny * size, 12 * nz * rows * ny),
        name="solve",
    )(part, *columns, *turned, *straight, eigen, shift)
    return ready, wh, wl


def filtered(wh, wl, straight, chunk, like):
    rows, nz, ny = wh.shape

    def body(wh_ref, wl_ref, zh_ref, zl_ref, *refs):
        scatter_row(refs, dot3(zh_ref[0], zl_ref[0], wh_ref[0], wl_ref[0]))

    w_spec = pl.BlockSpec((1, nz, ny), lambda i: (i, 0, 0))
    return pl.pallas_call(
        body,
        grid=(rows,),
        in_specs=[w_spec, w_spec] + [one_chunk(z, chunk) for z in straight],
        out_specs=[by_row(c) for c in like],
        out_shape=[jax.ShapeDtypeStruct(c.shape, f32) for c in like],
        cost_estimate=cost(6 * nz * rows * ny * straight[0].shape[1], 4 * nz * rows * ny),
        name="filtered",
    )(wh, wl, *straight)


def inverse(own, other, half, tables, planes, chunk, into, plain, step=2):
    lead, rows, _, ny = own[0].shape
    blocks = len(own) * lead
    nx = 2 * blocks * rows
    steps = GROUP // step
    extra = () if into is None else (into,)

    def body(half_ref, *refs):
        out_ref, f_ref = refs[-2:]
        yh_ref, yl_ref, xh_ref, xl_ref = refs[2 * len(own) : 2 * len(own) + 4]
        here = pl.program_id(0)

        @pl.when(here == 0)
        def _():
            for slot in range(2):
                for outer in range(len(own)):
                    for inner in range(lead):
                        block = outer * lead + inner
                        block = block if plain else half_ref[1] ^ block
                        first = ((half_ref[0] if slot == 0 else 1 - half_ref[0]) * blocks + block) * rows
                        for plane in range(GROUP):
                            value = refs[slot * len(own) + outer][inner, :, plane, :]
                            f_ref[plane, pl.ds(pl.multiple_of(first, rows), rows), :] = value

        for plane in range(step):
            fh, fl = split(f_ref[here * step + plane])
            hh, hl = split(dot3(fh, fl, yh_ref[...], yl_ref[...]))
            out_ref[plane] = dot3(xh_ref[...], xl_ref[...], hh, hl)

    operands = (half, *own, *other, *tables, *extra)
    return pl.pallas_call(
        body,
        grid=(steps,),
        in_specs=[smem()]
        + [whole(v.shape) for v in (*own, *other, *tables)]
        + [pl.BlockSpec(memory_space=pl.ANY) for _ in extra],
        out_specs=pl.BlockSpec((step, nx, ny), lambda i: (chunk * steps + i, 0, 0)),
        out_shape=jax.ShapeDtypeStruct((planes, nx, ny), f32),
        scratch_shapes=[pltpu.VMEM((GROUP, nx, ny), f32)],
        input_output_aliases={len(operands) - 1: 0} if extra else {},
        cost_estimate=cost(GROUP * 12 * nx * ny * nx, GROUP * nx * ny * 8),
        name="inverse",
    )(*operands)


def row_shift(first, rows, nx, ny):
    wave_x = (first + jnp.arange(rows, dtype=jnp.int32)).astype(f32)
    wave_y = jnp.arange(ny, dtype=jnp.int32).astype(f32)
    shift_x = 2.0 * jnp.sin(jnp.pi * wave_x / nx)
    shift_y = 2.0 * jnp.sin(jnp.pi * wave_y / ny)
    return shift_x[:, None] ** 2 + shift_y[None, :] ** 2


def swap(value):
    return lax.ppermute(value, "kpt", [(0, 1), (1, 0)])


def pairwise(value, distance):
    count = lax.axis_size("grid")
    return lax.ppermute(value, "grid", [(place, place ^ distance) for place in range(count)])


def across(parts, unit):
    return [parts[0]] + [pairwise(parts[n], n * unit) for n in range(1, len(parts))]


def turn(parts):
    _, rows, _, ny = parts[0].shape
    many = len(parts)

    def body(*refs):
        for b in range(parts[0].shape[0]):
            for a in range(many):
                refs[many + b][a] = refs[a][b]

    spec = [pl.BlockSpec((n, rows // 2, GROUP, ny), lambda i: (0, i, 0, 0)) for n in (parts[0].shape[0], many)]
    shape = jax.ShapeDtypeStruct((many, rows, GROUP, ny), f32)
    size = rows * GROUP * ny * many * parts[0].shape[0]
    return pl.pallas_call(
        body,
        grid=(2,),
        in_specs=[spec[0]] * many,
        out_specs=[spec[1]] * parts[0].shape[0],
        out_shape=[shape] * parts[0].shape[0],
        cost_estimate=cost(size * 100, size * 8),
        name="turn",
    )(*parts)


def exchange(value):
    return lax.all_to_all(value, "grid", split_axis=0, concat_axis=0, tiled=True)


def on_device_kernels(orbitals, kweights, occupations, z_basis, z_eigen):
    planes, nx, ny = orbitals.shape[3:]
    blocks = lax.axis_size("grid")
    rows = nx // (2 * blocks)
    chunks = planes // GROUP
    mine = lax.axis_index("kpt").astype(jnp.int32)
    half = jnp.stack([mine, lax.axis_index("grid").astype(jnp.int32)])
    table_x, scaled_x = real_basis(nx)
    table_y, scaled_y = real_basis(ny)
    to_modes = (*split_const(np.ascontiguousarray(table_y.T)), *split_const(table_x))
    to_grid = (*split_const(scaled_y), *split_const(np.ascontiguousarray(scaled_x.T)))

    columns = []
    for chunk in range(chunks):
        last = chunk == chunks - 1
        own, other = forward(orbitals, kweights, occupations, half, to_modes, chunk, blocks, last)
        if chunk == 0:
            z_basis, z_eigen, own = lax.optimization_barrier((z_basis, z_eigen, own))
        other = swap(other)
        if last:
            own = own + other
            columns.append([exchange(own)])
            break
        parts = [own[n : n + INNER] + other[n : n + INNER] for n in range(0, blocks, INNER)]
        parts = across(parts, INNER)
        parts = turn(parts)
        columns.append(across(parts, 1))
    zh, zl, th, tl = prepare(z_basis, half, blocks, planes)
    first = (mine * blocks + lax.axis_index("grid")) * rows
    shift = row_shift(first, rows, nx, ny)[:, None, :]
    part = None
    for chunk in range(chunks - 1):
        part = project(columns[chunk], (th, tl), chunk, part)
    if part is None:
        part = jnp.zeros((rows, planes * blocks, ny), f32)
    ready, wh, wl = solve(part, columns[-1], (zh, zl), (th, tl), z_eigen[:, None], shift, chunks - 1)
    out = None
    for chunk in range(chunks):
        if chunk == 0:
            own = [exchange(ready[0])]
        else:
            ready = filtered(wh, wl, (zh, zl), chunk, columns[0])
            parts = across(ready, 1)
            parts = turn(parts)
            own = across(parts, INNER)
        other = [swap(v) for v in own]
        out = inverse(own, other, half, to_grid, planes, chunk, out, chunk == 0)
    return out


precise = lax.Precision.HIGHEST


def on_device_plain(orbitals, kweights, occupations, z_basis, z_eigen):
    points, bands, _, planes, nx, ny = orbitals.shape
    blocks = lax.axis_size("grid")
    rows = nx // (2 * blocks)
    nz = planes * blocks
    mine = lax.axis_index("kpt")
    weights = (kweights[:, None] * occupations).astype(f32) / (16.0 * points * bands)
    values = orbitals.astype(f32)
    density = jnp.sum(weights[:, :, None, None, None, None] * values * values, axis=(0, 1, 2))
    table_x, scaled_x = (jnp.roll(jnp.asarray(t), -mine * (nx // 2), axis=0) for t in real_basis(nx))
    table_y, scaled_y = real_basis(ny)
    along = jnp.einsum("zxy,ky->zxk", density, table_y, precision=precise)
    spectrum = jnp.einsum("jx,zxk->jzk", table_x, along, precision=precise).reshape(2, blocks, rows, planes, ny)
    columns = exchange(spectrum[0] + swap(spectrum[1]))
    first = (mine * blocks + lax.axis_index("grid")) * rows
    factors = 1.0 / (z_eigen[:, None, None] + row_shift(first, rows, nx, ny)[None])
    by_plane = z_basis.reshape(blocks, planes, nz)
    projected = jnp.einsum("gpj,gapk->jak", by_plane, columns, precision=precise)
    filtered = jnp.einsum("gpj,jak->gapk", by_plane, projected * factors, precision=precise)
    own = exchange(filtered)
    modes = jnp.stack([own, swap(own)]).reshape(nx, planes, ny)
    half_done = jnp.einsum("jx,jzk->zxk", scaled_x, modes, precision=precise)
    return jnp.einsum("zxk,ky->zxy", half_done, scaled_y, precision=precise)


def whole_tiles(shape, blocks):
    planes, nx, ny = shape[3:]
    rows = nx // (2 * blocks)
    paired = blocks % INNER == 0 and blocks & (blocks - 1) == 0
    return paired and rows % 8 == 0 and ny % 128 == 0 and nx % 256 == 0 and planes % GROUP == 0


def on_device(orbitals, *rest):
    if not whole_tiles(orbitals.shape, lax.axis_size("grid")):
        return on_device_plain(orbitals, *rest)
    return on_device_kernels(orbitals, *rest)


def solution(mesh):
    step = jax.shard_map(
        on_device,
        mesh=mesh,
        in_specs=(P("kpt", None, None, "grid", None, None), P("kpt"), P("kpt", None), P(), P()),
        out_specs=P("grid", None, None),
        check_vma=False,
    )

    def run(orbitals, *rest):
        blocks = mesh.shape["grid"]
        local = list(orbitals.shape)
        local[3] //= blocks
        if not whole_tiles(local, blocks):
            return step(orbitals, *rest)
        return step(orbitals, *rest)

    return run
```

```python
import numpy as np
import jax
import jax.numpy as jnp
from jax import lax
from jax.experimental import pallas as pl
from jax.experimental.pallas import tpu as pltpu
from jax.sharding import PartitionSpec as P


f32 = jnp.float32
bf16 = jnp.bfloat16


def real_basis(length):
    position = np.arange(length)
    angles = (position[:, None] * position[None, :] % length) * (2.0 * np.pi / length)
    table = np.where(position[:, None] <= length // 2, np.cos(angles), np.sin(angles))
    edges = (position == 0) | (position == length // 2)
    weights = np.where(edges, 1.0, 2.0) / length
    return table.astype(np.float32), (table * weights[:, None]).astype(np.float32)


def split_const(table):
    high = table.astype(jnp.bfloat16)
    low = (table - high.astype(np.float32)).astype(jnp.bfloat16)
    return jnp.asarray(high), jnp.asarray(low)


def split(value):
    high = value.astype(bf16)
    return high, (value - high.astype(f32)).astype(bf16)


def dot3(ah, al, bh, bl):
    def one(a, b):
        return jnp.dot(a, b, preferred_element_type=f32)

    return one(ah, bh) + (one(ah, bl) + one(al, bh))


def whole(shape):
    zeros = (0,) * len(shape)
    return pl.BlockSpec(shape, lambda *_: zeros)


def smem():
    return pl.BlockSpec(memory_space=pltpu.SMEM)


def cost(flops, bytes_accessed):
    return pl.CostEstimate(flops=int(flops), bytes_accessed=int(bytes_accessed), transcendentals=0)


GROUP = 8
INNER = 4


def forward(orbitals, kweights, occupations, half, tables, chunk, blocks, plain, step=2):
    points, bands, parts, _, nx, ny = orbitals.shape
    rows = nx // (2 * blocks)
    steps = GROUP // step
    scale = 1.0 / (16.0 * points * bands)

    def body(half_ref, kweights_ref, occ_ref, orb_ref, yh_ref, yl_ref, xh_ref, xl_ref, own_ref, other_ref, s_ref):
        mine, place = half_ref[0], half_ref[1]
        here = pl.program_id(0)
        yh, yl = yh_ref[...], yl_ref[...]
        for plane in range(step):
            total = None
            for point in range(points):
                for band in range(bands):
                    weight = (kweights_ref[point] * occ_ref[point, band]).astype(f32) * scale
                    real = orb_ref[point, band, 0, plane].astype(f32)
                    imag = orb_ref[point, band, 1, plane].astype(f32)
                    term = weight * (real * real + imag * imag)
                    total = term if total is None else total + term
            dh, dl = split(total)
            ah, al = split(dot3(dh, dl, yh, yl))
            s_ref[here * step + plane] = dot3(xh_ref[...], xl_ref[...], ah, al)

        @pl.when(here == steps - 1)
        def _():
            for slot, out in ((0, own_ref), (1, other_ref)):
                for block in range(blocks):
                    first = ((mine if slot == 0 else 1 - mine) * blocks + (block if plain else place ^ block)) * rows
                    for plane in range(GROUP):
                        out[block, :, plane, :] = s_ref[plane, pl.ds(pl.multiple_of(first, rows), rows), :]

    out_shape = jax.ShapeDtypeStruct((blocks, rows, GROUP, ny), f32)
    return pl.pallas_call(
        body,
        grid=(steps,),
        in_specs=[smem(), smem(), smem()]
        + [pl.BlockSpec((points, bands, parts, step, nx, ny), lambda i: (0, 0, 0, chunk * steps + i, 0, 0))]
        + [whole(t.shape) for t in tables],
        out_specs=[whole(out_shape.shape)] * 2,
        out_shape=[out_shape] * 2,
        scratch_shapes=[pltpu.VMEM((GROUP, nx, ny), f32)],
        cost_estimate=cost(GROUP * 12 * nx * ny * nx, GROUP * nx * ny * 24),
        name="forward",
    )(half, kweights, occupations, orbitals, *tables)


def prepare(z_basis, half, blocks, planes):
    nz = z_basis.shape[0]
    chunks = planes // GROUP
    size = blocks * GROUP

    def body(half_ref, z_ref, zh_ref, zl_ref, th_ref, tl_ref):
        order = [outer * INNER + inner for inner in range(INNER) for outer in range(blocks // INNER)]
        here = pl.program_id(0)

        def rows_of(plain):
            places = [jnp.where(plain, n, half_ref[1] ^ block) for n, block in enumerate(order)]
            return jnp.concatenate([z_ref[place] for place in places], axis=0)

        zh_ref[0], zl_ref[0] = split(rows_of(here == 0))
        th_ref[...], tl_ref[...] = split(rows_of(here == chunks - 1).T)

    straight = jax.ShapeDtypeStruct((chunks, size, nz), bf16)
    turned = jax.ShapeDtypeStruct((nz, chunks * size), bf16)
    return pl.pallas_call(
        body,
        grid=(chunks,),
        in_specs=[smem(), pl.BlockSpec((blocks, GROUP, nz), lambda i: (0, i, 0))],
        out_specs=[pl.BlockSpec((1, size, nz), lambda i: (i, 0, 0))] * 2 + [pl.BlockSpec((nz, size), lambda i: (0, i))] * 2,
        out_shape=[straight] * 2 + [turned] * 2,
        cost_estimate=cost(nz * nz * 100, nz * nz * 12),
        name="prepare",
    )(half, z_basis.reshape(blocks, planes, nz))


def by_row(part):
    return pl.BlockSpec((part.shape[0], 1) + part.shape[2:], lambda i: (0, i, 0, 0))


def gather_row(refs, ny):
    return jnp.concatenate([ref[:, 0].reshape(-1, ny) for ref in refs], axis=0)


def scatter_row(refs, value):
    first = 0
    for ref in refs:
        size = ref.shape[0] * GROUP
        ref[:, 0] = value[first : first + size].reshape(ref.shape[0], GROUP, value.shape[1])
        first += size


def one_chunk(table, chunk):
    return pl.BlockSpec((1,) + table.shape[1:], lambda i: (chunk, 0, 0))


def project(columns, turned, start, span, before):
    rows, _, ny = columns[0].shape[1:]
    nz = turned[0].shape[0]
    size = sum(c.shape[0] for c in columns) * GROUP
    many = len(columns)
    extra = () if before is None else (before,)

    def body(*refs):
        xh, xl = split(gather_row(refs[:many], ny))
        value = dot3(refs[many][...], refs[many + 1][...], xh, xl)
        refs[-1][0] = value if before is None else value + refs[many + 2][0]

    part = pl.BlockSpec((1, nz, ny), lambda i: (i, 0, 0))
    return pl.pallas_call(
        body,
        grid=(rows,),
        in_specs=[by_row(c) for c in columns] + [pl.BlockSpec((nz, size), lambda i: (0, start // span)) for _ in turned] + [part for _ in extra],
        out_specs=part,
        out_shape=jax.ShapeDtypeStruct((rows, nz, ny), f32),
        cost_estimate=cost(6 * nz * size * rows * ny, 8 * nz * rows * ny),
        name="project",
    )(*columns, *turned, *extra)


def solve(part, columns, straight, turned, eigen, shift, start, span):
    rows, _, ny = columns[0].shape[1:]
    nz = turned[0].shape[0]
    size = sum(c.shape[0] for c in columns) * GROUP
    many = len(columns)

    def body(part_ref, *refs):
        th_ref, tl_ref, zh_ref, zl_ref, e_ref, s_ref = refs[many : many + 6]
        wh_ref, wl_ref = refs[-2:]
        xh, xl = split(gather_row(refs[:many], ny))
        projected = part_ref[0] + dot3(th_ref[...], tl_ref[...], xh, xl)
        wh, wl = split(projected / (e_ref[...] + s_ref[0]))
        wh_ref[0], wl_ref[0] = wh, wl
        scatter_row(refs[many + 6 : -2], dot3(zh_ref[0], zl_ref[0], wh, wl))

    w_spec = pl.BlockSpec((1, nz, ny), lambda i: (i, 0, 0))
    w_shape = jax.ShapeDtypeStruct((rows, nz, ny), bf16)
    *ready, wh, wl = pl.pallas_call(
        body,
        grid=(rows,),
        in_specs=[w_spec]
        + [by_row(c) for c in columns]
        + [pl.BlockSpec((nz, size), lambda i: (0, start // span)) for _ in turned]
        + [one_chunk(z, 0) for z in straight]
        + [whole(eigen.shape), pl.BlockSpec((1, 1, ny), lambda i: (i, 0, 0))],
        out_specs=[by_row(columns[-1]), w_spec, w_spec],
        out_shape=[jax.ShapeDtypeStruct(columns[-1].shape, f32), w_shape, w_shape],
        cost_estimate=cost(12 * nz * rows * ny * size, 12 * nz * rows * ny),
        name="solve",
    )(part, *columns, *turned, *straight, eigen, shift)
    return ready, wh, wl


def filtered(wh, wl, straight, chunk, like):
    rows, nz, ny = wh.shape

    def body(wh_ref, wl_ref, zh_ref, zl_ref, *refs):
        scatter_row(refs, dot3(zh_ref[0], zl_ref[0], wh_ref[0], wl_ref[0]))

    w_spec = pl.BlockSpec((1, nz, ny), lambda i: (i, 0, 0))
    return pl.pallas_call(
        body,
        grid=(rows,),
        in_specs=[w_spec, w_spec] + [one_chunk(z, chunk) for z in straight],
        out_specs=[by_row(c) for c in like],
        out_shape=[jax.ShapeDtypeStruct(c.shape, f32) for c in like],
        cost_estimate=cost(6 * nz * rows * ny * straight[0].shape[1], 4 * nz * rows * ny),
        name="filtered",
    )(wh, wl, *straight)


def inverse(own, other, half, tables, planes, chunk, into, plain, step=2):
    lead, rows, _, ny = own[0].shape
    blocks = len(own) * lead
    nx = 2 * blocks * rows
    steps = GROUP // step
    extra = () if into is None else (into,)

    def body(half_ref, *refs):
        out_ref, f_ref = refs[-2:]
        yh_ref, yl_ref, xh_ref, xl_ref = refs[2 * len(own) : 2 * len(own) + 4]
        here = pl.program_id(0)

        @pl.when(here == 0)
        def _():
            for slot in range(2):
                for outer in range(len(own)):
                    for inner in range(lead):
                        block = outer * lead + inner
                        block = block if plain else half_ref[1] ^ block
                        first = ((half_ref[0] if slot == 0 else 1 - half_ref[0]) * blocks + block) * rows
                        for plane in range(GROUP):
                            value = refs[slot * len(own) + outer][inner, :, plane, :]
                            f_ref[plane, pl.ds(pl.multiple_of(first, rows), rows), :] = value

        for plane in range(step):
            fh, fl = split(f_ref[here * step + plane])
            hh, hl = split(dot3(fh, fl, yh_ref[...], yl_ref[...]))
            out_ref[plane] = dot3(xh_ref[...], xl_ref[...], hh, hl)

    operands = (half, *own, *other, *tables, *extra)
    return pl.pallas_call(
        body,
        grid=(steps,),
        in_specs=[smem()]
        + [whole(v.shape) for v in (*own, *other, *tables)]
        + [pl.BlockSpec(memory_space=pl.ANY) for _ in extra],
        out_specs=pl.BlockSpec((step, nx, ny), lambda i: (chunk * steps + i, 0, 0)),
        out_shape=jax.ShapeDtypeStruct((planes, nx, ny), f32),
        scratch_shapes=[pltpu.VMEM((GROUP, nx, ny), f32)],
        input_output_aliases={len(operands) - 1: 0} if extra else {},
        cost_estimate=cost(GROUP * 12 * nx * ny * nx, GROUP * nx * ny * 8),
        name="inverse",
    )(*operands)


def row_shift(first, rows, nx, ny):
    wave_x = (first + jnp.arange(rows, dtype=jnp.int32)).astype(f32)
    wave_y = jnp.arange(ny, dtype=jnp.int32).astype(f32)
    shift_x = 2.0 * jnp.sin(jnp.pi * wave_x / nx)
    shift_y = 2.0 * jnp.sin(jnp.pi * wave_y / ny)
    return shift_x[:, None] ** 2 + shift_y[None, :] ** 2


def swap(value):
    return lax.ppermute(value, "kpt", [(0, 1), (1, 0)])


def pairwise(value, distance):
    count = lax.axis_size("grid")
    return lax.ppermute(value, "grid", [(place, place ^ distance) for place in range(count)])


def across(parts, unit):
    return [parts[0]] + [pairwise(parts[n], n * unit) for n in range(1, len(parts))]


def turn(parts):
    _, rows, _, ny = parts[0].shape
    many = len(parts)

    def body(*refs):
        for b in range(parts[0].shape[0]):
            for a in range(many):
                refs[many + b][a] = refs[a][b]

    spec = [pl.BlockSpec((n, rows // 2, GROUP, ny), lambda i: (0, i, 0, 0)) for n in (parts[0].shape[0], many)]
    shape = jax.ShapeDtypeStruct((many, rows, GROUP, ny), f32)
    size = rows * GROUP * ny * many * parts[0].shape[0]
    return pl.pallas_call(
        body,
        grid=(2,),
        in_specs=[spec[0]] * many,
        out_specs=[spec[1]] * parts[0].shape[0],
        out_shape=[shape] * parts[0].shape[0],
        cost_estimate=cost(size * 100, size * 8),
        name="turn",
    )(*parts)


def exchange(value):
    return lax.all_to_all(value, "grid", split_axis=0, concat_axis=0, tiled=True)


def on_device_kernels(orbitals, kweights, occupations, z_basis, z_eigen):
    planes, nx, ny = orbitals.shape[3:]
    blocks = lax.axis_size("grid")
    rows = nx // (2 * blocks)
    chunks = planes // GROUP
    mine = lax.axis_index("kpt").astype(jnp.int32)
    half = jnp.stack([mine, lax.axis_index("grid").astype(jnp.int32)])
    table_x, scaled_x = real_basis(nx)
    table_y, scaled_y = real_basis(ny)
    to_modes = (*split_const(np.ascontiguousarray(table_y.T)), *split_const(table_x))
    to_grid = (*split_const(scaled_y), *split_const(np.ascontiguousarray(scaled_x.T)))

    columns = []
    for chunk in range(chunks):
        last = chunk == chunks - 1
        own, other = forward(orbitals, kweights, occupations, half, to_modes, chunk, blocks, last)
        if chunk == 0:
            z_basis, z_eigen, own = lax.optimization_barrier((z_basis, z_eigen, own))
        other = swap(other)
        if last:
            own = own + other
            columns.append([exchange(own)])
            break
        parts = [own[n : n + INNER] + other[n : n + INNER] for n in range(0, blocks, INNER)]
        parts = across(parts, INNER)
        parts = turn(parts)
        columns.append(across(parts, 1))
    zh, zl, th, tl = prepare(z_basis, half, blocks, planes)
    first = (mine * blocks + lax.axis_index("grid")) * rows
    shift = row_shift(first, rows, nx, ny)[:, None, :]
    part = None
    tail = 2 - chunks % 2
    for chunk in range(0, chunks - tail, 2):
        part = project(columns[chunk] + columns[chunk + 1], (th, tl), chunk, 2, part)
    if part is None:
        part = jnp.zeros((rows, planes * blocks, ny), f32)
    ready, wh, wl = solve(part, sum(columns[-tail:], []), (zh, zl), (th, tl), z_eigen[:, None], shift, chunks - tail, tail)
    out = None
    for chunk in range(chunks):
        if chunk == 0:
            own = [exchange(ready[0])]
        else:
            ready = filtered(wh, wl, (zh, zl), chunk, columns[0])
            parts = across(ready, 1)
            parts = turn(parts)
            own = across(parts, INNER)
        other = [swap(v) for v in own]
        out = inverse(own, other, half, to_grid, planes, chunk, out, chunk == 0)
    return out


precise = lax.Precision.HIGHEST


def on_device_plain(orbitals, kweights, occupations, z_basis, z_eigen):
    points, bands, _, planes, nx, ny = orbitals.shape
    blocks = lax.axis_size("grid")
    rows = nx // (2 * blocks)
    nz = planes * blocks
    mine = lax.axis_index("kpt")
    weights = (kweights[:, None] * occupations).astype(f32) / (16.0 * points * bands)
    values = orbitals.astype(f32)
    density = jnp.sum(weights[:, :, None, None, None, None] * values * values, axis=(0, 1, 2))
    table_x, scaled_x = (jnp.roll(jnp.asarray(t), -mine * (nx // 2), axis=0) for t in real_basis(nx))
    table_y, scaled_y = real_basis(ny)
    along = jnp.einsum("zxy,ky->zxk", density, table_y, precision=precise)
    spectrum = jnp.einsum("jx,zxk->jzk", table_x, along, precision=precise).reshape(2, blocks, rows, planes, ny)
    columns = exchange(spectrum[0] + swap(spectrum[1]))
    first = (mine * blocks + lax.axis_index("grid")) * rows
    factors = 1.0 / (z_eigen[:, None, None] + row_shift(first, rows, nx, ny)[None])
    by_plane = z_basis.reshape(blocks, planes, nz)
    projected = jnp.einsum("gpj,gapk->jak", by_plane, columns, precision=precise)
    filtered = jnp.einsum("gpj,jak->gapk", by_plane, projected * factors, precision=precise)
    own = exchange(filtered)
    modes = jnp.stack([own, swap(own)]).reshape(nx, planes, ny)
    half_done = jnp.einsum("jx,jzk->zxk", scaled_x, modes, precision=precise)
    return jnp.einsum("zxk,ky->zxy", half_done, scaled_y, precision=precise)


def whole_tiles(shape, blocks):
    planes, nx, ny = shape[3:]
    rows = nx // (2 * blocks)
    paired = blocks % INNER == 0 and blocks & (blocks - 1) == 0
    return paired and rows % 8 == 0 and ny % 128 == 0 and nx % 256 == 0 and planes % GROUP == 0


def on_device(orbitals, *rest):
    if not whole_tiles(orbitals.shape, lax.axis_size("grid")):
        return on_device_plain(orbitals, *rest)
    return on_device_kernels(orbitals, *rest)


def solution(mesh):
    step = jax.shard_map(
        on_device,
        mesh=mesh,
        in_specs=(P("kpt", None, None, "grid", None, None), P("kpt"), P("kpt", None), P(), P()),
        out_specs=P("grid", None, None),
        check_vma=False,
    )

    def run(orbitals, *rest):
        blocks = mesh.shape["grid"]
        local = list(orbitals.shape)
        local[3] //= blocks
        if not whole_tiles(local, blocks):
            return step(orbitals, *rest)
        return step(orbitals, *rest)

    return run
```

```python
import numpy as np
import jax
import jax.numpy as jnp
from jax import lax
from jax.experimental import pallas as pl
from jax.experimental.pallas import tpu as pltpu
from jax.sharding import PartitionSpec as P


f32 = jnp.float32
bf16 = jnp.bfloat16


def real_basis(length):
    position = np.arange(length)
    angles = (position[:, None] * position[None, :] % length) * (2.0 * np.pi / length)
    table = np.where(position[:, None] <= length // 2, np.cos(angles), np.sin(angles))
    edges = (position == 0) | (position == length // 2)
    weights = np.where(edges, 1.0, 2.0) / length
    return table.astype(np.float32), (table * weights[:, None]).astype(np.float32)


def split_const(table):
    high = table.astype(jnp.bfloat16)
    low = (table - high.astype(np.float32)).astype(jnp.bfloat16)
    return jnp.asarray(high), jnp.asarray(low)


def split(value):
    high = value.astype(bf16)
    return high, (value - high.astype(f32)).astype(bf16)


def dot3(ah, al, bh, bl):
    def one(a, b):
        return jnp.dot(a, b, preferred_element_type=f32)

    size = ah.shape[0]
    both = one(jnp.concatenate([ah, al], axis=0), bh)
    return both[:size] + (both[size:] + one(ah, bl))


def whole(shape):
    zeros = (0,) * len(shape)
    return pl.BlockSpec(shape, lambda *_: zeros)


def smem():
    return pl.BlockSpec(memory_space=pltpu.SMEM)


def cost(flops, bytes_accessed):
    return pl.CostEstimate(flops=int(flops), bytes_accessed=int(bytes_accessed), transcendentals=0)


GROUP = 8
INNER = 4
PAIR = 4


def forward(orbitals, kweights, occupations, half, tables, chunk, blocks, plain, step=4):
    points, bands, parts, _, nx, ny = orbitals.shape
    rows = nx // (2 * blocks)
    steps = GROUP // step
    scale = 1.0 / (16.0 * points * bands)

    def body(half_ref, kweights_ref, occ_ref, orb_ref, yh_ref, yl_ref, xh_ref, xl_ref, own_ref, other_ref, s_ref):
        mine, place = half_ref[0], half_ref[1]
        here = pl.program_id(0)
        yh, yl = yh_ref[...], yl_ref[...]
        for plane in range(step):
            total = None
            for point in range(points):
                for band in range(bands):
                    weight = (kweights_ref[point] * occ_ref[point, band]).astype(f32) * scale
                    real = orb_ref[point, band, 0, plane].astype(f32)
                    imag = orb_ref[point, band, 1, plane].astype(f32)
                    term = weight * (real * real + imag * imag)
                    total = term if total is None else total + term
            dh, dl = split(total)
            ah, al = split(dot3(dh, dl, yh, yl))
            s_ref[here * step + plane] = dot3(xh_ref[...], xl_ref[...], ah, al)

        @pl.when(here == steps - 1)
        def _():
            for slot, out in ((0, own_ref), (1, other_ref)):
                for block in range(blocks):
                    first = ((mine if slot == 0 else 1 - mine) * blocks + (block if plain else place ^ block)) * rows
                    out[block] = jnp.swapaxes(s_ref[:, pl.ds(pl.multiple_of(first, rows), rows), :], 0, 1)

    out_shape = jax.ShapeDtypeStruct((blocks, rows, GROUP, ny), f32)
    return pl.pallas_call(
        body,
        grid=(steps,),
        in_specs=[smem(), smem(), smem()]
        + [pl.BlockSpec((points, bands, parts, step, nx, ny), lambda i: (0, 0, 0, chunk * steps + i, 0, 0))]
        + [whole(t.shape) for t in tables],
        out_specs=[whole(out_shape.shape)] * 2,
        out_shape=[out_shape] * 2,
        scratch_shapes=[pltpu.VMEM((GROUP, nx, ny), f32)],
        cost_estimate=cost(GROUP * 12 * nx * ny * nx, GROUP * nx * ny * 24),
        name="forward",
    )(half, kweights, occupations, orbitals, *tables)


def prepare(z_basis, half, blocks, planes):
    nz = z_basis.shape[0]
    chunks = planes // GROUP
    size = blocks * GROUP

    def body(half_ref, z_ref, zh_ref, zl_ref, th_ref, tl_ref):
        order = [outer * INNER + inner for inner in range(INNER) for outer in range(blocks // INNER)]
        here = pl.program_id(0)

        def rows_of(plain):
            places = [jnp.where(plain, n, half_ref[1] ^ block) for n, block in enumerate(order)]
            return jnp.concatenate([z_ref[place] for place in places], axis=0)

        zh_ref[0], zl_ref[0] = split(rows_of(here == 0))
        th_ref[...], tl_ref[...] = split(rows_of(here == chunks - 1).T)

    straight = jax.ShapeDtypeStruct((chunks, size, nz), bf16)
    turned = jax.ShapeDtypeStruct((nz, chunks * size), bf16)
    return pl.pallas_call(
        body,
        grid=(chunks,),
        in_specs=[smem(), pl.BlockSpec((blocks, GROUP, nz), lambda i: (0, i, 0))],
        out_specs=[pl.BlockSpec((1, size, nz), lambda i: (i, 0, 0))] * 2 + [pl.BlockSpec((nz, size), lambda i: (0, i))] * 2,
        out_shape=[straight] * 2 + [turned] * 2,
        cost_estimate=cost(nz * nz * 100, nz * nz * 12),
        name="prepare",
    )(half, z_basis.reshape(blocks, planes, nz))


def by_row(part):
    return pl.BlockSpec((part.shape[0], PAIR) + part.shape[2:], lambda i: (0, i, 0, 0))


def gather_row(refs, row, ny):
    return jnp.concatenate([ref[:, row].reshape(-1, ny) for ref in refs], axis=0)


def scatter_row(refs, row, value):
    first = 0
    for ref in refs:
        size = ref.shape[0] * GROUP
        ref[:, row] = value[first : first + size].reshape(ref.shape[0], GROUP, value.shape[1])
        first += size


def one_chunk(table, chunk):
    return pl.BlockSpec((1,) + table.shape[1:], lambda i: (chunk, 0, 0))


def project(columns, turned, start, span, before):
    rows, _, ny = columns[0].shape[1:]
    nz = turned[0].shape[0]
    size = sum(c.shape[0] for c in columns) * GROUP
    many = len(columns)
    extra = () if before is None else (before,)

    def body(*refs):
        for row in range(PAIR):
            xh, xl = split(gather_row(refs[:many], row, ny))
            value = dot3(refs[many][...], refs[many + 1][...], xh, xl)
            refs[-1][row] = value if before is None else value + refs[many + 2][row]

    part = pl.BlockSpec((PAIR, nz, ny), lambda i: (i, 0, 0))
    return pl.pallas_call(
        body,
        grid=(rows // PAIR,),
        in_specs=[by_row(c) for c in columns] + [pl.BlockSpec((nz, size), lambda i: (0, start // span)) for _ in turned] + [part for _ in extra],
        out_specs=part,
        out_shape=jax.ShapeDtypeStruct((rows, nz, ny), f32),
        cost_estimate=cost(6 * nz * size * rows * ny, 8 * nz * rows * ny),
        name="project",
    )(*columns, *turned, *extra)


def solve(part, columns, straight, turned, eigen, shift, start, span):
    rows, _, ny = columns[0].shape[1:]
    nz = turned[0].shape[0]
    size = sum(c.shape[0] for c in columns) * GROUP
    many = len(columns)

    def body(part_ref, *refs):
        th_ref, tl_ref, zh_ref, zl_ref, e_ref, s_ref = refs[many : many + 6]
        wh_ref, wl_ref = refs[-2:]
        for row in range(PAIR):
            xh, xl = split(gather_row(refs[:many], row, ny))
            projected = part_ref[row] + dot3(th_ref[...], tl_ref[...], xh, xl)
            wh, wl = split(projected / (e_ref[...] + s_ref[row]))
            wh_ref[row], wl_ref[row] = wh, wl
            scatter_row(refs[many + 6 : -2], row, dot3(zh_ref[0], zl_ref[0], wh, wl))

    w_spec = pl.BlockSpec((PAIR, nz, ny), lambda i: (i, 0, 0))
    w_shape = jax.ShapeDtypeStruct((rows, nz, ny), bf16)
    *ready, wh, wl = pl.pallas_call(
        body,
        grid=(rows // PAIR,),
        in_specs=[w_spec]
        + [by_row(c) for c in columns]
        + [pl.BlockSpec((nz, size), lambda i: (0, start // span)) for _ in turned]
        + [one_chunk(z, 0) for z in straight]
        + [whole(eigen.shape), pl.BlockSpec((PAIR, 1, ny), lambda i: (i, 0, 0))],
        out_specs=[by_row(columns[-1]), w_spec, w_spec],
        out_shape=[jax.ShapeDtypeStruct(columns[-1].shape, f32), w_shape, w_shape],
        cost_estimate=cost(12 * nz * rows * ny * size, 12 * nz * rows * ny),
        name="solve",
    )(part, *columns, *turned, *straight, eigen, shift)
    return ready, wh, wl


def filtered(wh, wl, straight, chunk, like):
    rows, nz, ny = wh.shape

    def body(wh_ref, wl_ref, zh_ref, zl_ref, *refs):
        for row in range(PAIR):
            scatter_row(refs, row, dot3(zh_ref[0], zl_ref[0], wh_ref[row], wl_ref[row]))

    w_spec = pl.BlockSpec((PAIR, nz, ny), lambda i: (i, 0, 0))
    return pl.pallas_call(
        body,
        grid=(rows // PAIR,),
        in_specs=[w_spec, w_spec] + [one_chunk(z, chunk) for z in straight],
        out_specs=[by_row(c) for c in like],
        out_shape=[jax.ShapeDtypeStruct(c.shape, f32) for c in like],
        cost_estimate=cost(6 * nz * rows * ny * straight[0].shape[1], 4 * nz * rows * ny),
        name="filtered",
    )(wh, wl, *straight)


def inverse(own, other, half, tables, planes, chunk, into, plain, step=4):
    lead, rows, _, ny = own[0].shape
    blocks = len(own) * lead
    nx = 2 * blocks * rows
    steps = GROUP // step
    extra = () if into is None else (into,)

    def body(half_ref, *refs):
        out_ref, f_ref = refs[-2:]
        yh_ref, yl_ref, xh_ref, xl_ref = refs[2 * len(own) : 2 * len(own) + 4]
        here = pl.program_id(0)

        @pl.when(here == 0)
        def _():
            for slot in range(2):
                for outer in range(len(own)):
                    for inner in range(lead):
                        block = outer * lead + inner
                        block = block if plain else half_ref[1] ^ block
                        first = ((half_ref[0] if slot == 0 else 1 - half_ref[0]) * blocks + block) * rows
                        value = jnp.swapaxes(refs[slot * len(own) + outer][inner], 0, 1)
                        f_ref[:, pl.ds(pl.multiple_of(first, rows), rows), :] = value

        for plane in range(step):
            fh, fl = split(f_ref[here * step + plane])
            hh, hl = split(dot3(fh, fl, yh_ref[...], yl_ref[...]))
            out_ref[plane] = dot3(xh_ref[...], xl_ref[...], hh, hl)

    operands = (half, *own, *other, *tables, *extra)
    return pl.pallas_call(
        body,
        grid=(steps,),
        in_specs=[smem()]
        + [whole(v.shape) for v in (*own, *other, *tables)]
        + [pl.BlockSpec(memory_space=pl.ANY) for _ in extra],
        out_specs=pl.BlockSpec((step, nx, ny), lambda i: (chunk * steps + i, 0, 0)),
        out_shape=jax.ShapeDtypeStruct((planes, nx, ny), f32),
        scratch_shapes=[pltpu.VMEM((GROUP, nx, ny), f32)],
        input_output_aliases={len(operands) - 1: 0} if extra else {},
        cost_estimate=cost(GROUP * 12 * nx * ny * nx, GROUP * nx * ny * 8),
        name="inverse",
    )(*operands)


def row_shift(first, rows, nx, ny):
    wave_x = (first + jnp.arange(rows, dtype=jnp.int32)).astype(f32)
    wave_y = jnp.arange(ny, dtype=jnp.int32).astype(f32)
    shift_x = 2.0 * jnp.sin(jnp.pi * wave_x / nx)
    shift_y = 2.0 * jnp.sin(jnp.pi * wave_y / ny)
    return shift_x[:, None] ** 2 + shift_y[None, :] ** 2


def swap(value):
    return lax.ppermute(value, "kpt", [(0, 1), (1, 0)])


def pairwise(value, distance):
    count = lax.axis_size("grid")
    return lax.ppermute(value, "grid", [(place, place ^ distance) for place in range(count)])


def across(parts, unit):
    return [parts[0]] + [pairwise(parts[n], n * unit) for n in range(1, len(parts))]


def turn(parts):
    _, rows, _, ny = parts[0].shape
    many = len(parts)

    def body(*refs):
        for b in range(parts[0].shape[0]):
            for a in range(many):
                refs[many + b][a] = refs[a][b]

    spec = [pl.BlockSpec((n, rows // 2, GROUP, ny), lambda i: (0, i, 0, 0)) for n in (parts[0].shape[0], many)]
    shape = jax.ShapeDtypeStruct((many, rows, GROUP, ny), f32)
    size = rows * GROUP * ny * many * parts[0].shape[0]
    return pl.pallas_call(
        body,
        grid=(2,),
        in_specs=[spec[0]] * many,
        out_specs=[spec[1]] * parts[0].shape[0],
        out_shape=[shape] * parts[0].shape[0],
        cost_estimate=cost(size * 100, size * 8),
        name="turn",
    )(*parts)


def exchange(value):
    return lax.all_to_all(value, "grid", split_axis=0, concat_axis=0, tiled=True)


def on_device_kernels(orbitals, kweights, occupations, z_basis, z_eigen):
    planes, nx, ny = orbitals.shape[3:]
    blocks = lax.axis_size("grid")
    rows = nx // (2 * blocks)
    chunks = planes // GROUP
    mine = lax.axis_index("kpt").astype(jnp.int32)
    half = jnp.stack([mine, lax.axis_index("grid").astype(jnp.int32)])
    table_x, scaled_x = real_basis(nx)
    table_y, scaled_y = real_basis(ny)
    to_modes = (*split_const(np.ascontiguousarray(table_y.T)), *split_const(table_x))
    to_grid = (*split_const(scaled_y), *split_const(np.ascontiguousarray(scaled_x.T)))

    columns = []
    for chunk in range(chunks):
        last = chunk == chunks - 1
        own, other = forward(orbitals, kweights, occupations, half, to_modes, chunk, blocks, last)
        if chunk == 0:
            z_basis, z_eigen, own = lax.optimization_barrier((z_basis, z_eigen, own))
        other = swap(other)
        if last:
            own = own + other
            columns.append([exchange(own)])
            break
        parts = [own[n : n + INNER] + other[n : n + INNER] for n in range(0, blocks, INNER)]
        parts = across(parts, INNER)
        parts = turn(parts)
        columns.append(across(parts, 1))
    zh, zl, th, tl = prepare(z_basis, half, blocks, planes)
    first = (mine * blocks + lax.axis_index("grid")) * rows
    shift = row_shift(first, rows, nx, ny)[:, None, :]
    part = None
    tail = 2 - chunks % 2
    for chunk in range(0, chunks - tail, 2):
        part = project(columns[chunk] + columns[chunk + 1], (th, tl), chunk, 2, part)
    if part is None:
        part = jnp.zeros((rows, planes * blocks, ny), f32)
    ready, wh, wl = solve(part, sum(columns[-tail:], []), (zh, zl), (th, tl), z_eigen[:, None], shift, chunks - tail, tail)
    out = None
    for chunk in range(chunks):
        if chunk == 0:
            own = [exchange(ready[0])]
        else:
            ready = filtered(wh, wl, (zh, zl), chunk, columns[0])
            parts = across(ready, 1)
            parts = turn(parts)
            own = across(parts, INNER)
        other = [swap(v) for v in own]
        out = inverse(own, other, half, to_grid, planes, chunk, out, chunk == 0)
    return out


precise = lax.Precision.HIGHEST


def on_device_plain(orbitals, kweights, occupations, z_basis, z_eigen):
    points, bands, _, planes, nx, ny = orbitals.shape
    blocks = lax.axis_size("grid")
    rows = nx // (2 * blocks)
    nz = planes * blocks
    mine = lax.axis_index("kpt")
    weights = (kweights[:, None] * occupations).astype(f32) / (16.0 * points * bands)
    values = orbitals.astype(f32)
    density = jnp.sum(weights[:, :, None, None, None, None] * values * values, axis=(0, 1, 2))
    table_x, scaled_x = (jnp.roll(jnp.asarray(t), -mine * (nx // 2), axis=0) for t in real_basis(nx))
    table_y, scaled_y = real_basis(ny)
    along = jnp.einsum("zxy,ky->zxk", density, table_y, precision=precise)
    spectrum = jnp.einsum("jx,zxk->jzk", table_x, along, precision=precise).reshape(2, blocks, rows, planes, ny)
    columns = exchange(spectrum[0] + swap(spectrum[1]))
    first = (mine * blocks + lax.axis_index("grid")) * rows
    factors = 1.0 / (z_eigen[:, None, None] + row_shift(first, rows, nx, ny)[None])
    by_plane = z_basis.reshape(blocks, planes, nz)
    projected = jnp.einsum("gpj,gapk->jak", by_plane, columns, precision=precise)
    filtered = jnp.einsum("gpj,jak->gapk", by_plane, projected * factors, precision=precise)
    own = exchange(filtered)
    modes = jnp.stack([own, swap(own)]).reshape(nx, planes, ny)
    half_done = jnp.einsum("jx,jzk->zxk", scaled_x, modes, precision=precise)
    return jnp.einsum("zxk,ky->zxy", half_done, scaled_y, precision=precise)


def whole_tiles(shape, blocks):
    planes, nx, ny = shape[3:]
    rows = nx // (2 * blocks)
    paired = blocks % INNER == 0 and blocks & (blocks - 1) == 0
    return paired and rows % 8 == 0 and ny % 128 == 0 and nx % 256 == 0 and planes % GROUP == 0


def on_device(orbitals, *rest):
    if not whole_tiles(orbitals.shape, lax.axis_size("grid")):
        return on_device_plain(orbitals, *rest)
    return on_device_kernels(orbitals, *rest)


def solution(mesh):
    step = jax.shard_map(
        on_device,
        mesh=mesh,
        in_specs=(P("kpt", None, None, "grid", None, None), P("kpt"), P("kpt", None), P(), P()),
        out_specs=P("grid", None, None),
        check_vma=False,
    )

    def run(orbitals, *rest):
        blocks = mesh.shape["grid"]
        local = list(orbitals.shape)
        local[3] //= blocks
        if not whole_tiles(local, blocks):
            return step(orbitals, *rest)
        return step(orbitals, *rest)

    return run
```
